32 devices in a mesh: tile: 16 (over z, x, core), mem: 2 (over y).
Axes of the slice: x: 2, y: 2, z: 4, core: 2. Of those that a mesh axis runs over, the one named last changes fastest.
Arguments:
- anomalies: bfloat16 [80, 137, 2048], P('mem', None, 'tile'), may hold values from -6 to 6
- analysis_weights: bfloat16 [16, 80, 80], P('tile'), may hold values from -0.6 to 1.7
- background_mean: bfloat16 [137, 2048], P(None, 'tile'), may hold values from -6 to 6
- background: bfloat16 [80, 137, 2048], P('mem', None, 'tile'), may hold values from -6 to 6
- jacobian_table: bfloat16 [8461, 137], replicated, may hold values from -0.5 to 0.5
- channel_list: int32 [96], replicated, may hold values from 0 to 8460
- send_slots: int32 [16, 16, 32], P('tile'), may hold values from -1 to 127, as said below
- footprint: int32 [8192, 4], P('tile'), may hold values from 0 to 511, as said below
- footprint_weight: bfloat16 [8192, 4], P('tile'), may hold values from 0.25 to 1
- channel_bias: float32 [96], replicated, may hold values from -4 to 4
Outputs:
- analysis_members: bfloat16 [80, 137, 2048], P('mem', None, 'tile')
- radiance_prior: float32 [96, 80, 8192], P(None, 'mem', 'tile')
The draws below stay inside these ranges and needn't reach their ends.
Inputs may be any that keep to these rules, and one draw needn't show every extreme that they name: `send_slots`: entry [s, d, i] is a column within owner s's block of 128 columns that owner s sends to tile d in slot i, or -1 for an empty slot; the filled slots of a pair come first, each pair fills 1 to 32 slots, and in every draw one tile receives 32 filled slots from every owner. `footprint`: entry [o, j] is a slot of the buffer of observation o's tile, which holds 32 slots from each owner in owner order; every entry names a filled slot, the 4 entries of a row differ, and every filled slot is named by some row of that tile.
All inputs are finite; a program needn't handle non-finite values.
Results may differ from the reference program's by a relative error of at most 0.0021.
Values may be sent and summed in bfloat16 or wider, within the bound.
No kernel may reach another device: no remote copies, remote signals or barrier semaphores. Data moves between devices by JAX's collectives and lax.ppermute only.
A program may use at most 128 MiB of HBM per device.

```python
import math
import jax
import jax.numpy as jnp
from jax import lax

MEMBERS = 80
LEVELS = 137
SPECTRUM = 8461
CHANNELS = 96
COLS_DEV = 128
GROUP = 128
SLOTS = 32
OBS_DEV = 512
FOOT = 4
COLUMNS = 2048
POINTS = 16
OBSERVATIONS = 8192
N_TILE = 16


def draw_analysis_weights(key, part):
    identity = jnp.eye(MEMBERS, dtype=jnp.float32)[None]
    noise_draw = jnp.clip(jax.random.normal(jax.random.fold_in(key, 1), (POINTS, MEMBERS, MEMBERS), jnp.float32), -4.0, 4.0)
    diag_part = identity
    return (diag_part + noise_draw * (0.6 / math.sqrt(MEMBERS))).astype(jnp.bfloat16)


def slot_counts(key):
    tile_count = COLUMNS // COLS_DEV
    uniform_part = jax.random.randint(jax.random.fold_in(key, 11), (tile_count, tile_count), 1, SLOTS + 1)
    receiver_load = jax.random.randint(jax.random.fold_in(key, 12), (1, tile_count), 1, 5)
    counts = jnp.clip(uniform_part * receiver_load // 3, 1, SLOTS)
    full_receiver = jax.random.randint(jax.random.fold_in(key, 13), (), 0, tile_count)
    counts = jnp.where(jnp.arange(tile_count)[None, :] == full_receiver, SLOTS, counts)
    return counts.astype(jnp.int32)


def draw_send_slots(key, part):
    tile_count = COLUMNS // COLS_DEV
    counts = slot_counts(key)
    columns = jax.random.randint(jax.random.fold_in(key, 14), (tile_count, tile_count, SLOTS), 0, COLS_DEV)
    filled = jnp.arange(SLOTS)[None, None, :] < counts[:, :, None]
    return jnp.where(filled, columns, -1).astype(jnp.int32)


def draw_footprint(key, part):
    tile_count = COLUMNS // COLS_DEV
    buffer_size = tile_count * SLOTS
    counts = slot_counts(key)
    filled = jnp.arange(SLOTS)[None, None, :] < jnp.transpose(counts)[:, :, None]
    filled = filled.reshape(tile_count, buffer_size)
    receiver_keys = jax.random.split(jax.random.fold_in(key, 15), tile_count)

    def shuffle_one(subkey):
        return jax.random.permutation(subkey, buffer_size).astype(jnp.int32)
    shuffle = jax.vmap(shuffle_one)(receiver_keys)
    scores = jnp.where(filled, shuffle, buffer_size + shuffle)
    slot_order = jnp.argsort(scores, axis=1, stable=True).astype(jnp.int32)
    filled_count = jnp.sum(filled.astype(jnp.int32), axis=1, keepdims=True)
    position = jnp.arange(OBS_DEV * FOOT, dtype=jnp.int32)[None, :] % filled_count
    foot_slots = jnp.take_along_axis(slot_order, position, axis=1)
    return foot_slots.reshape(tile_count * OBS_DEV, FOOT).astype(jnp.int32)


def set_ends(entries, stream_key, low, high):
    longest = entries.shape.index(max(entries.shape))
    spots = []
    for shift in (0, 1):
        where = [jax.random.randint(jax.random.fold_in(stream_key, axis), (), 0, length) for axis, length in enumerate(entries.shape)]
        where[longest] = (where[longest] + shift) % entries.shape[longest]
        spots.append(tuple(where))
    return entries.at[spots[0]].set(low).at[spots[1]].set(high)


def levels(key, extent, shards, low, largest):
    factor_of = 1.0
    for dim, parts in shards:
        draws = jax.random.uniform(jax.random.fold_in(jax.random.fold_in(key, 6), dim), (parts,), jnp.float32, low / len(shards), largest / len(shards))
        factor_of = factor_of * jnp.repeat(jnp.exp(draws), extent[dim] // parts).reshape((-1,) + (1,) * (len(extent) - 1 - dim))
    return factor_of


def gaussian(rng, shape, scale, limit, shards=(), kind=jnp.bfloat16):
    values = scale * jax.random.normal(rng, shape, jnp.float32)
    if shards:
        values = values * levels(rng, shape, shards, -0.22, 0.18)
    return jnp.clip(values, -limit, limit).astype(kind)


def setup_inputs(seed: int = 0) -> dict:
    key_list = jax.random.split(jax.random.key(seed), 11)
    anomalies = gaussian(key_list[0], (MEMBERS, LEVELS, COLUMNS), 1.0, 6.0, ((0, 2), (2, 16)))
    analysis_weights = draw_analysis_weights(jax.random.fold_in(key_list[10], 71), 0)
    background_mean = gaussian(key_list[2], (LEVELS, COLUMNS), 1.0, 6.0, ((1, 16),))
    background = gaussian(key_list[3], (MEMBERS, LEVELS, COLUMNS), 1.0, 6.0, ((0, 2), (2, 16)))
    jacobian_table = gaussian(key_list[4], (SPECTRUM, LEVELS), LEVELS ** -0.5, 0.5)
    channel_list = set_ends(jax.random.randint(key_list[5], (CHANNELS,), 0, SPECTRUM), jax.random.fold_in(key_list[5], 1), 0, SPECTRUM - 1).astype(jnp.int32)
    send_slots = draw_send_slots(jax.random.fold_in(key_list[10], 71), 0)
    footprint = draw_footprint(jax.random.fold_in(key_list[10], 71), 0)
    footprint_weight = jnp.clip(jnp.exp(math.log(1.0) - 1.3862944 * jax.random.uniform(key_list[8], (OBSERVATIONS, FOOT), jnp.float32) ** levels(key_list[8], (OBSERVATIONS, FOOT), ((0, 16),), -0.2, 0.2)), 0.25, 1.0).astype(jnp.bfloat16)
    channel_bias = gaussian(key_list[9], (CHANNELS,), 1.0, 4.0, (), jnp.float32)
    return {"anomalies": anomalies, "analysis_weights": analysis_weights, "background_mean": background_mean, "background": background, "jacobian_table": jacobian_table, "channel_list": channel_list, "send_slots": send_slots, "footprint": footprint, "footprint_weight": footprint_weight, "channel_bias": channel_bias}


def reference(anomalies, analysis_weights, background_mean, background, jacobian_table, channel_list, send_slots, footprint, footprint_weight, channel_bias):
    points = analysis_weights.shape[0]
    shaped = anomalies.astype(jnp.float32).reshape(MEMBERS, LEVELS, points, GROUP)
    mixture = jnp.einsum('klgc,gkm->mlgc', shaped, analysis_weights.astype(jnp.float32))
    mixture = mixture.reshape(MEMBERS, LEVELS, points * GROUP)
    analysis_members = (background_mean.astype(jnp.float32)[None] + mixture).astype(jnp.bfloat16)

    selected = jnp.take(jacobian_table, channel_list, axis=0).astype(jnp.float32)
    foot_slots = footprint.reshape(N_TILE, OBS_DEV, FOOT)
    foot_weight = footprint_weight.astype(jnp.float32).reshape(N_TILE, OBS_DEV, FOOT)

    def per_receiver(receiver):
        slot_ids = lax.dynamic_index_in_dim(foot_slots, receiver, 0, keepdims=False)
        weight = lax.dynamic_index_in_dim(foot_weight, receiver, 0, keepdims=False)
        source = (slot_ids // SLOTS).astype(jnp.int32)
        slot_place = (slot_ids % SLOTS).astype(jnp.int32)
        local_col = send_slots[source, receiver, slot_place]
        column = (source * COLS_DEV + local_col).astype(jnp.int32)
        profiles = jnp.take(background, column.reshape(-1), axis=2).astype(jnp.float32)
        radiance = jnp.einsum('cl,kls->cks', selected, profiles).astype(jnp.bfloat16)
        radiance = lax.optimization_barrier(radiance).astype(jnp.float32)
        radiance = radiance.reshape(CHANNELS, MEMBERS, OBS_DEV, FOOT)
        combined = jnp.sum(radiance * weight[None, None], axis=3)
        return combined + channel_bias.astype(jnp.float32)[:, None, None]

    stacked = lax.map(per_receiver, jnp.arange(N_TILE, dtype=jnp.int32))
    radiance_prior = jnp.transpose(stacked, (1, 2, 0, 3)).reshape(CHANNELS, MEMBERS, N_TILE * OBS_DEV)
    return analysis_members, radiance_prior
```

```python
import functools

import jax
import jax.numpy as jnp
from jax import lax
from jax.experimental import pallas as pl
from jax.experimental.pallas import tpu as pltpu
from jax.sharding import PartitionSpec as P

LANES = 128
SPLIT = (3, 3)


def one_hot(index, count, dtype=jnp.bfloat16):
    return (index[..., None] == lax.iota(jnp.int32, count)).astype(dtype)


def dot(spec, a, b):
    return jnp.einsum(spec, a, b, preferred_element_type=jnp.float32)


def pack_kernel(hot_ref, own_ref, *out_refs):
    packed = jnp.dot(
        hot_ref[...], own_ref[...], preferred_element_type=jnp.float32
    ).astype(jnp.bfloat16)
    slots = out_refs[0].shape[0]
    for d, out_ref in enumerate(out_refs):
        out_ref[...] = packed[d * slots : (d + 1) * slots]


def pack(hot, own, slots, first, block, count):
    columns_dev = own.shape[0]
    partners = hot.shape[0] // slots
    rows = count * block
    return list(
        pl.pallas_call(
            pack_kernel,
            grid=(count,),
            in_specs=[
                pl.BlockSpec(hot.shape, lambda i: (0, 0)),
                pl.BlockSpec((columns_dev, block), lambda i: (0, first + i)),
            ],
            out_specs=[pl.BlockSpec((slots, block), lambda i: (0, i))] * partners,
            out_shape=[jax.ShapeDtypeStruct((slots, rows), own.dtype)] * partners,
            cost_estimate=pl.CostEstimate(
                flops=2 * hot.size * rows,
                bytes_accessed=2 * rows * (columns_dev + hot.shape[0]),
                transcendentals=0,
            ),
            name="pack",
        )(hot, own)
    )


def prior_kernel(first, block, mem_dev, sources, bias_ref, spread_ref, *refs):
    out_ref = refs[-1]
    rows = jnp.concatenate([ref[...] for ref in refs[:sources]], axis=0)
    total = lax.dot_general(
        rows,
        spread_ref[...],
        (((0,), (0,)), ((), ())),
        preferred_element_type=jnp.float32,
    )
    channel = (first + pl.program_id(0)) * block
    for c in range(block):
        out_ref[c] = total[c * mem_dev : (c + 1) * mem_dev] + bias_ref[channel + c]


def prior_piece(shape, block, first, count, near, far, spread, bias, so_far):
    _, mem_dev, obs_count = shape
    width = block * mem_dev
    slots, all_slots = near[0].shape[0], spread.shape[0]
    in_specs = [
        pl.BlockSpec(memory_space=pltpu.SMEM),
        pl.BlockSpec(spread.shape, lambda i: (0, 0)),
        *[pl.BlockSpec((slots, width), lambda i: (0, first + i))] * len(near),
        *[pl.BlockSpec((far[0].shape[0], width), lambda i: (0, i))] * len(far),
    ]
    operands = [bias, spread, *near, *far]
    aliases = {}
    if so_far is not None:
        aliases = {len(operands): 0}
        in_specs.append(pl.BlockSpec(memory_space=pl.ANY))
        operands.append(so_far)
    return pl.pallas_call(
        functools.partial(prior_kernel, first, block, mem_dev, len(near) + len(far)),
        grid=(count,),
        in_specs=in_specs,
        out_specs=pl.BlockSpec((block, mem_dev, obs_count), lambda i: (first + i, 0, 0)),
        out_shape=jax.ShapeDtypeStruct(shape, jnp.float32),
        input_output_aliases=aliases,
        cost_estimate=pl.CostEstimate(
            flops=2 * all_slots * width * count * obs_count,
            bytes_accessed=2 * width * count * (all_slots + 2 * obs_count),
            transcendentals=0,
        ),
        name="prior",
    )(*operands)


def pieces_of(channels, mem_dev):
    for block in range(1, channels // 2 + 1):
        if channels % block == 0 and block * mem_dev % LANES == 0:
            total = channels // block
            relay = max(1, total * SPLIT[0] // sum(SPLIT))
            return block, relay, total - relay
    return channels, 1, 0


def shards(
    n_tile,
    n_mem,
    anomalies,
    analysis_weights,
    background_mean,
    background,
    jacobian_table,
    channel_list,
    send_slots,
    footprint,
    footprint_weight,
    channel_bias,
):
    mem_dev, _, columns_dev = anomalies.shape
    spectrum = jacobian_table.shape[0]
    channels = channel_list.shape[0]
    slots = send_slots.shape[2]
    obs_count, foot = footprint.shape
    half = n_tile // 2
    half_slots = half * slots
    me = lax.axis_index("tile")
    mine = lax.axis_index("mem")
    my_half = me // half
    halves = [[h * half + i for i in range(half)] for h in range(2)]
    mirror = [(i, (i + half) % n_tile) for i in range(n_tile)]
    block, relay, direct = pieces_of(channels, mem_dev)
    width = block * mem_dev

    place = me % half
    partners = jnp.stack([me ^ d for d in range(n_tile)])
    partner_cols = jnp.take(send_slots[0], partners, axis=0, mode="clip")
    far_cols = lax.dynamic_slice_in_dim(send_slots[0], (1 - my_half) * half, half, 0)
    relay_cols = lax.ppermute(far_cols, "tile", mirror)

    picks = one_hot(channel_list, spectrum)
    selected = dot("cs,sl->cl", picks, jacobian_table).astype(jnp.bfloat16)
    owned = dot("cl,klx->ckx", selected, background).astype(jnp.bfloat16)
    owned = owned.reshape(channels * mem_dev, columns_dev)
    identity = jnp.eye(columns_dev, dtype=jnp.bfloat16)
    hot = lax.optimization_barrier(one_hot(partner_cols.reshape(-1), columns_dev))
    relay_hot = lax.optimization_barrier(one_hot(relay_cols.reshape(-1), columns_dev))

    own = dot("sx,rx->sr", identity, owned[: relay * width]).astype(jnp.bfloat16)
    seen = lax.ppermute(own, "tile", mirror)
    own = dot("sx,rx->sr", identity, owned).astype(jnp.bfloat16)

    def to_partner(array, d):
        return lax.ppermute(array, "tile", [(i, i ^ d) for i in range(n_tile)])

    near = pack(hot[:half_slots], own, slots, 0, relay * width, 1 + (direct == relay))
    near[1:] = [to_partner(near[d], d) for d in range(1, half)]
    far = []
    if direct:
        far = pack(hot[half_slots:], own, slots, 1, relay * width, 1)
        far = [to_partner(far[d], half + d) for d in range(half)]

    places = footprint.T
    weights = footprint_weight.T
    near_place = places - my_half * half_slots
    far_place = places - (1 - my_half) * half_slots
    mixed_place = jnp.stack([near_place ^ (place * slots), far_place])
    spread = sum(
        jnp.where(
            mixed_place[:, None, j] == lax.iota(jnp.int32, half_slots)[None, :, None],
            weights[j],
            jnp.zeros((), weights.dtype),
        )
        for j in range(foot)
    ).reshape(2 * half_slots, obs_count)

    relayed = dot("sx,xr->sr", relay_hot, seen).astype(jnp.bfloat16)
    relayed = lax.all_to_all(
        relayed, "tile", 0, 0, tiled=True, axis_index_groups=halves
    )
    shape = (channels, mem_dev, obs_count)
    prior = None
    if direct:
        direct_spread = jnp.take(
            spread.reshape(n_tile, slots, obs_count),
            jnp.concatenate([jnp.arange(half), half + (jnp.arange(half) ^ place)]),
            axis=0,
            mode="clip",
        ).reshape(spread.shape)
        prior = prior_piece(
            shape, block, relay, direct, near, far, direct_spread, channel_bias, None
        )
    prior = prior_piece(
        shape, block, 0, relay, near, [relayed], spread, channel_bias, prior
    )

    weight_cols = lax.dynamic_slice_in_dim(analysis_weights[0], mine * mem_dev, mem_dev, 1)
    mixture = background_mean.astype(jnp.float32)[None]
    for shift in range(n_mem):
        piece = anomalies
        if shift:
            piece = lax.ppermute(
                anomalies, "mem", [((i + shift) % n_mem, i) for i in range(n_mem)]
            )
        start = lax.rem(mine + shift, n_mem) * mem_dev
        part = lax.dynamic_slice_in_dim(weight_cols, start, mem_dev, 0)
        mixture = mixture + dot("klc,km->mlc", piece, part)
    mixture = mixture.astype(jnp.bfloat16)
    return mixture, prior


def solution(mesh):
    sizes = dict(mesh.shape)
    placed = (
        P("mem", None, "tile"),
        P("tile", None, None),
        P(None, "tile"),
        P("mem", None, "tile"),
        P(),
        P(),
        P("tile", None, None),
        P("tile", None),
        P("tile", None),
        P(),
    )

    def body(*arrays):
        return shards(sizes["tile"], sizes["mem"], *arrays)

    return jax.shard_map(
        body,
        mesh=mesh,
        in_specs=placed,
        out_specs=(P("mem", None, "tile"), P(None, "mem", "tile")),
        check_vma=False,
    )
```

```python
import functools

import jax
import jax.numpy as jnp
from jax import lax
from jax.experimental import pallas as pl
from jax.experimental.pallas import tpu as pltpu
from jax.sharding import PartitionSpec as P

LANES = 128
SPLIT = (2, 2, 2)


def one_hot(index, count, dtype=jnp.bfloat16):
    return (index[..., None] == lax.iota(jnp.int32, count)).astype(dtype)


def dot(spec, a, b):
    return jnp.einsum(spec, a, b, preferred_element_type=jnp.float32)


def pack_kernel(sends, relays, me_ref, slot_ref, owned_ref, *out_refs):
    columns_dev = owned_ref.shape[1]
    slots = slot_ref.shape[1]
    named = jnp.concatenate(
        [slot_ref[pl.ds(me_ref[0] ^ d, 1), :] for d, _, _ in sends], axis=1
    )
    column = lax.broadcasted_iota(jnp.int32, (columns_dev, named.shape[1]), 0)
    hot = jnp.where(column == named, 1.0, 0.0).T.astype(jnp.bfloat16)
    own = owned_ref[...].T
    for first, stop in dict.fromkeys(send[1:] for send in sends):
        picked = [n for n, send in enumerate(sends) if send[1:] == (first, stop)]
        rows = hot[picked[0] * slots : (picked[-1] + 1) * slots]
        packed = jnp.dot(rows, own[:, first:stop], preferred_element_type=jnp.float32)
        packed = packed.astype(jnp.bfloat16)
        for k, n in enumerate(picked):
            out_refs[n][...] = packed[k * slots : (k + 1) * slots]
    for (first, stop), ref in zip(relays, out_refs[len(sends) :]):
        ref[...] = own[:, first:stop]


def pack(me, send_slots, owned, sends, relays):
    rows, columns_dev = owned.shape
    slots = send_slots.shape[1]
    shapes = [(slots, stop - first) for _, first, stop in sends]
    shapes += [(columns_dev, stop - first) for first, stop in relays]
    outs = pl.pallas_call(
        functools.partial(pack_kernel, sends, relays),
        in_specs=[
            pl.BlockSpec(memory_space=pltpu.SMEM),
            pl.BlockSpec(memory_space=pltpu.VMEM),
            pl.BlockSpec(memory_space=pltpu.VMEM),
        ],
        out_specs=[pl.BlockSpec(memory_space=pltpu.VMEM)] * len(shapes),
        out_shape=[jax.ShapeDtypeStruct(shape, owned.dtype) for shape in shapes],
        cost_estimate=pl.CostEstimate(
            flops=2 * len(sends) * slots * columns_dev * rows,
            bytes_accessed=2 * rows * (2 * columns_dev + len(sends) * slots),
            transcendentals=0,
        ),
        name="pack",
    )(me, send_slots, owned)
    return list(outs[: len(sends)]), list(outs[len(sends) :])


def relay_kernel(hot_ref, *refs):
    start = 0
    for ref in refs[:-1]:
        stop = start + ref.shape[1]
        refs[-1][:, start:stop] = jnp.dot(
            hot_ref[...], ref[...], preferred_element_type=jnp.float32
        ).astype(jnp.bfloat16)
        start = stop


def relay_pack(hot, pieces):
    width = sum(piece.shape[1] for piece in pieces)
    return pl.pallas_call(
        relay_kernel,
        out_shape=jax.ShapeDtypeStruct((hot.shape[0], width), jnp.bfloat16),
        cost_estimate=pl.CostEstimate(
            flops=2 * hot.size * width,
            bytes_accessed=2 * width * sum(hot.shape),
            transcendentals=0,
        ),
        name="relay",
    )(hot, *pieces)


def prior_kernel(
    first, count, block, mem_dev, sources, bias_ref, place_ref, spread_ref, *refs
):
    prior_ref, table_ref, done_ref, sems = refs[-4:]

    start = 0
    for side in range(2):
        rows = spread_ref.shape[0] // 2 // sources[side]
        for d in range(sources[side]):
            at = side * rows * sources[side]
            if sources[side] > 1:
                at = pl.multiple_of(at + (place_ref[0] ^ d) * rows, rows)
            table_ref[start : start + rows] = spread_ref[pl.ds(at, rows)]
            start += rows

    width = block * mem_dev
    copies = []
    for i in range(count):
        lanes = slice(i * width, (i + 1) * width)
        rows = jnp.concatenate([ref[:, lanes] for ref in refs[: sum(sources)]], axis=0)
        total = lax.dot_general(
            rows,
            table_ref[...],
            (((0,), (0,)), ((), ())),
            preferred_element_type=jnp.float32,
        )
        for c in range(block):
            bias = bias_ref[(first + i) * block + c]
            done_ref[i, c] = total[c * mem_dev : (c + 1) * mem_dev] + bias
        copies.append(
            pltpu.make_async_copy(
                done_ref.at[i],
                prior_ref.at[pl.ds((first + i) * block, block)],
                sems.at[i],
            )
        )
        copies[-1].start()
    for copy in copies:
        copy.wait()


def prior_piece(shape, block, first, count, near, far, spread, bias, place, so_far):
    _, mem_dev, obs_count = shape
    width = count * block * mem_dev
    slots, all_slots = near[0].shape[0], spread.shape[0]
    in_specs = [
        pl.BlockSpec(memory_space=pltpu.SMEM),
        pl.BlockSpec(memory_space=pltpu.SMEM),
        pl.BlockSpec(memory_space=pltpu.VMEM),
        *[pl.BlockSpec((slots, width), lambda i: (0, first // count))] * len(near),
        *[pl.BlockSpec(memory_space=pltpu.VMEM)] * len(far),
    ]
    operands = [bias, place, spread, *near, *far]
    aliases = {}
    if so_far is not None:
        aliases = {len(operands): 0}
        in_specs.append(pl.BlockSpec(memory_space=pl.ANY))
        operands.append(so_far)
    return pl.pallas_call(
        functools.partial(
            prior_kernel, first, count, block, mem_dev, (len(near), len(far))
        ),
        grid=(1,),
        in_specs=in_specs,
        out_specs=pl.BlockSpec(memory_space=pl.ANY),
        out_shape=jax.ShapeDtypeStruct(shape, jnp.float32),
        scratch_shapes=[
            pltpu.VMEM(spread.shape, spread.dtype),
            pltpu.VMEM((count, block, mem_dev, obs_count), jnp.float32),
            pltpu.SemaphoreType.DMA((count,)),
        ],
        input_output_aliases=aliases,
        cost_estimate=pl.CostEstimate(
            flops=2 * all_slots * width * obs_count,
            bytes_accessed=2 * width * (all_slots + 2 * obs_count),
            transcendentals=0,
        ),
        name="prior",
    )(*operands)


def pieces_of(channels, mem_dev):
    for block in range(1, channels // 2 + 1):
        if channels % block == 0 and block * mem_dev % LANES == 0:
            if sum(SPLIT) * block == channels:
                return block, SPLIT
            return block, (channels // block, 0)
    return channels, (1, 0)


def shards(
    n_tile,
    n_mem,
    anomalies,
    analysis_weights,
    background_mean,
    background,
    jacobian_table,
    channel_list,
    send_slots,
    footprint,
    footprint_weight,
    channel_bias,
):
    mem_dev, _, columns_dev = anomalies.shape
    spectrum = jacobian_table.shape[0]
    channels = channel_list.shape[0]
    slots = send_slots.shape[2]
    obs_count, foot = footprint.shape
    half = n_tile // 2
    half_slots = half * slots
    me = lax.axis_index("tile")
    mine = lax.axis_index("mem")
    my_half = me // half
    halves = [[h * half + i for i in range(half)] for h in range(2)]
    mirror = [(i, (i + half) % n_tile) for i in range(n_tile)]
    block, split = pieces_of(channels, mem_dev)
    relay, direct = sum(split[:-1]), split[-1]

    place = me % half
    far_cols = lax.dynamic_slice_in_dim(send_slots[0], (1 - my_half) * half, half, 0)
    relay_cols = lax.ppermute(far_cols, "tile", mirror)

    picks = one_hot(channel_list, spectrum)
    selected = dot("cs,sl->cl", picks, jacobian_table).astype(jnp.bfloat16)
    selected = lax.optimization_barrier(selected)
    owned = dot("cl,klx->ckx", selected, background).astype(jnp.bfloat16)
    owned = owned.reshape(channels * mem_dev, columns_dev)
    relay_hot = lax.optimization_barrier(one_hot(relay_cols.reshape(-1), columns_dev))

    def to_partner(array, d):
        return lax.ppermute(array, "tile", [(i, i ^ d) for i in range(n_tile)])

    windows, first = [], 0
    for count in split:
        windows.append((first, first + count * block * mem_dev))
        first = windows[-1][1]
    total = first
    args = me[None], send_slots[0], owned
    early = range(half // 2, half)
    late = [d for d in range(half) if d not in early]
    direct_to = range(half, n_tile) if direct else ()
    near = [None] * half
    sent, seen = pack(*args, [(d, 0, total) for d in early], windows[:1])
    for d, array in zip(early, sent):
        near[d] = array
    sent, more = pack(
        *args,
        [(d, 0, total) for d in late] + [(d, *windows[-1]) for d in direct_to],
        windows[1:-1],
    )
    for d, array in zip(late, sent):
        near[d] = array
    far = sent[len(late) :]
    seen = seen + more
    for i in range(len(seen)):
        seen[i] = lax.ppermute(seen[i], "tile", mirror)
    near[1:] = [to_partner(near[d], d) for d in range(1, half)]
    far = [to_partner(far[d], half + d) for d in range(len(far))]

    places = footprint.T
    weights = footprint_weight.T
    near_place = places - my_half * half_slots
    far_place = places - (1 - my_half) * half_slots
    mixed_place = jnp.stack([near_place, far_place])
    spread = sum(
        jnp.where(
            mixed_place[:, None, j] == lax.iota(jnp.int32, half_slots)[None, :, None],
            weights[j],
            jnp.zeros((), weights.dtype),
        )
        for j in range(foot)
    ).reshape(2 * half_slots, obs_count)

    shape = (channels, mem_dev, obs_count)
    relayed = relay_pack(relay_hot, seen)
    relayed = lax.all_to_all(
        relayed, "tile", 0, 0, tiled=True, axis_index_groups=halves
    )
    prior = None
    for first, count, others in ((relay, direct, far), (0, relay, [relayed])):
        if count:
            prior = prior_piece(
                shape, block, first, count, near, others,
                spread, channel_bias, place[None], prior,
            )

    weight_cols = lax.dynamic_slice_in_dim(analysis_weights[0], mine * mem_dev, mem_dev, 1)
    mixture = background_mean.astype(jnp.float32)[None]
    for shift in range(n_mem):
        piece = anomalies
        if shift:
            piece = lax.ppermute(
                anomalies, "mem", [((i + shift) % n_mem, i) for i in range(n_mem)]
            )
        start = lax.rem(mine + shift, n_mem) * mem_dev
        part = lax.dynamic_slice_in_dim(weight_cols, start, mem_dev, 0)
        mixture = mixture + dot("klc,km->mlc", piece, part)
    mixture = mixture.astype(jnp.bfloat16)
    return mixture, prior


def solution(mesh):
    sizes = dict(mesh.shape)
    placed = (
        P("mem", None, "tile"),
        P("tile", None, None),
        P(None, "tile"),
        P("mem", None, "tile"),
        P(),
        P(),
        P("tile", None, None),
        P("tile", None),
        P("tile", None),
        P(),
    )

    def body(*arrays):
        return shards(sizes["tile"], sizes["mem"], *arrays)

    return jax.shard_map(
        body,
        mesh=mesh,
        in_specs=placed,
        out_specs=(P("mem", None, "tile"), P(None, "mem", "tile")),
        check_vma=False,
    )
```

```python
import functools

import jax
import jax.numpy as jnp
from jax import lax
from jax.experimental import pallas as pl
from jax.experimental.pallas import tpu as pltpu
from jax.sharding import PartitionSpec as P

LANES = 128
SPLIT = (2, 2, 2)


def one_hot(index, count, dtype=jnp.bfloat16):
    return (index[..., None] == lax.iota(jnp.int32, count)).astype(dtype)


def dot(spec, a, b):
    return jnp.einsum(spec, a, b, preferred_element_type=jnp.float32)


def pack_kernel(sends, relays, me_ref, slot_ref, owned_ref, *out_refs):
    columns_dev = owned_ref.shape[1]
    slots = slot_ref.shape[1]
    named = jnp.concatenate(
        [slot_ref[pl.ds(me_ref[0] ^ d, 1), :] for d, _, _ in sends], axis=1
    )
    column = lax.broadcasted_iota(jnp.int32, (columns_dev, named.shape[1]), 0)
    hot = jnp.where(column == named, 1.0, 0.0).T.astype(jnp.bfloat16)
    own = owned_ref[...].T
    for first, stop in dict.fromkeys(send[1:] for send in sends):
        picked = [n for n, send in enumerate(sends) if send[1:] == (first, stop)]
        rows = hot[picked[0] * slots : (picked[-1] + 1) * slots]
        packed = jnp.dot(rows, own[:, first:stop], preferred_element_type=jnp.float32)
        packed = packed.astype(jnp.bfloat16)
        for k, n in enumerate(picked):
            out_refs[n][...] = packed[k * slots : (k + 1) * slots]
    for (first, stop), ref in zip(relays, out_refs[len(sends) :]):
        ref[...] = own[:, first:stop]


def pack(me, send_slots, owned, sends, relays):
    rows, columns_dev = owned.shape
    slots = send_slots.shape[1]
    shapes = [(slots, stop - first) for _, first, stop in sends]
    shapes += [(columns_dev, stop - first) for first, stop in relays]
    outs = pl.pallas_call(
        functools.partial(pack_kernel, sends, relays),
        in_specs=[
            pl.BlockSpec(memory_space=pltpu.SMEM),
            pl.BlockSpec(memory_space=pltpu.VMEM),
            pl.BlockSpec(memory_space=pltpu.VMEM),
        ],
        out_specs=[pl.BlockSpec(memory_space=pltpu.VMEM)] * len(shapes),
        out_shape=[jax.ShapeDtypeStruct(shape, owned.dtype) for shape in shapes],
        cost_estimate=pl.CostEstimate(
            flops=2 * len(sends) * slots * columns_dev * rows,
            bytes_accessed=2 * rows * (2 * columns_dev + len(sends) * slots),
            transcendentals=0,
        ),
        name="pack",
    )(me, send_slots, owned)
    return list(outs[: len(sends)]), list(outs[len(sends) :])


def relay_kernel(hot_ref, *refs):
    start = 0
    for ref in refs[:-1]:
        stop = start + ref.shape[1]
        refs[-1][:, start:stop] = jnp.dot(
            hot_ref[...], ref[...], preferred_element_type=jnp.float32
        ).astype(jnp.bfloat16)
        start = stop


def relay_pack(hot, pieces):
    width = sum(piece.shape[1] for piece in pieces)
    return pl.pallas_call(
        relay_kernel,
        out_shape=jax.ShapeDtypeStruct((hot.shape[0], width), jnp.bfloat16),
        cost_estimate=pl.CostEstimate(
            flops=2 * hot.size * width,
            bytes_accessed=2 * width * sum(hot.shape),
            transcendentals=0,
        ),
        name="relay",
    )(hot, *pieces)


def prior_kernel(
    first, count, block, mem_dev, sources, bias_ref, place_ref, spread_ref, *refs
):
    prior_ref, table_ref, done_ref, sems, far_ref, far_sems = refs[-6:]
    width = block * mem_dev
    spans = [slice(i * width, (i + 1) * width) for i in range(count)]
    near_refs, far_refs, loads = refs[: sources[0]], refs[sources[0] : sum(sources)], []
    if sources[1] == 1:
        for i, span in enumerate(spans):
            at = (slice(None), span)
            loads.append(
                pltpu.make_async_copy(far_refs[0].at[at], far_ref.at[at], far_sems.at[i])
            )
            loads[-1].start()
        far_refs = (far_ref,)

    start = 0
    for side in range(2):
        rows = spread_ref.shape[0] // 2 // sources[side]
        for d in range(sources[side]):
            at = side * rows * sources[side]
            if sources[side] > 1:
                at = pl.multiple_of(at + (place_ref[0] ^ d) * rows, rows)
            table_ref[start : start + rows] = spread_ref[pl.ds(at, rows)]
            start += rows

    copies = []
    for i, span in enumerate(spans):
        if loads:
            loads[i].wait()
        rows = jnp.concatenate([ref[:, span] for ref in (*near_refs, *far_refs)], axis=0)
        total = lax.dot_general(
            rows,
            table_ref[...],
            (((0,), (0,)), ((), ())),
            preferred_element_type=jnp.float32,
        )
        for c in range(block):
            bias = bias_ref[(first + i) * block + c]
            done_ref[i, c] = total[c * mem_dev : (c + 1) * mem_dev] + bias
        copies.append(
            pltpu.make_async_copy(
                done_ref.at[i],
                prior_ref.at[pl.ds((first + i) * block, block)],
                sems.at[i],
            )
        )
        copies[-1].start()
    for copy in copies:
        copy.wait()


def prior_piece(shape, block, first, count, near, far, spread, bias, place, so_far):
    _, mem_dev, obs_count = shape
    width = count * block * mem_dev
    slots, all_slots = near[0].shape[0], spread.shape[0]
    in_specs = [
        pl.BlockSpec(memory_space=pltpu.SMEM),
        pl.BlockSpec(memory_space=pltpu.SMEM),
        pl.BlockSpec(memory_space=pltpu.VMEM),
        *[pl.BlockSpec((slots, width), lambda i: (0, first // count))] * len(near),
        *[pl.BlockSpec(memory_space=pl.ANY if len(far) == 1 else pltpu.VMEM)] * len(far),
    ]
    operands = [bias, place, spread, *near, *far]
    aliases = {}
    if so_far is not None:
        aliases = {len(operands): 0}
        in_specs.append(pl.BlockSpec(memory_space=pl.ANY))
        operands.append(so_far)
    return pl.pallas_call(
        functools.partial(
            prior_kernel, first, count, block, mem_dev, (len(near), len(far))
        ),
        grid=(1,),
        in_specs=in_specs,
        out_specs=pl.BlockSpec(memory_space=pl.ANY),
        out_shape=jax.ShapeDtypeStruct(shape, jnp.float32),
        scratch_shapes=[
            pltpu.VMEM(spread.shape, spread.dtype),
            pltpu.VMEM((count, block, mem_dev, obs_count), jnp.float32),
            pltpu.SemaphoreType.DMA((count,)),
            pltpu.VMEM(far[0].shape, far[0].dtype),
            pltpu.SemaphoreType.DMA((count,)),
        ],
        input_output_aliases=aliases,
        cost_estimate=pl.CostEstimate(
            flops=2 * all_slots * width * obs_count,
            bytes_accessed=2 * width * (all_slots + 2 * obs_count),
            transcendentals=0,
        ),
        name="prior",
    )(*operands)


def pieces_of(channels, mem_dev):
    for block in range(1, channels // 2 + 1):
        if channels % block == 0 and block * mem_dev % LANES == 0:
            if sum(SPLIT) * block == channels:
                return block, SPLIT
            return block, (channels // block, 0)
    return channels, (1, 0)


def shards(
    n_tile,
    n_mem,
    anomalies,
    analysis_weights,
    background_mean,
    background,
    jacobian_table,
    channel_list,
    send_slots,
    footprint,
    footprint_weight,
    channel_bias,
):
    mem_dev, _, columns_dev = anomalies.shape
    spectrum = jacobian_table.shape[0]
    channels = channel_list.shape[0]
    slots = send_slots.shape[2]
    obs_count, foot = footprint.shape
    half = n_tile // 2
    half_slots = half * slots
    me = lax.axis_index("tile")
    mine = lax.axis_index("mem")
    my_half = me // half
    halves = [[h * half + i for i in range(half)] for h in range(2)]
    mirror = [(i, (i + half) % n_tile) for i in range(n_tile)]
    block, split = pieces_of(channels, mem_dev)
    relay, direct = sum(split[:-1]), split[-1]

    place = me % half
    far_cols = lax.dynamic_slice_in_dim(send_slots[0], (1 - my_half) * half, half, 0)
    relay_cols = lax.ppermute(far_cols, "tile", mirror)

    picks = one_hot(channel_list, spectrum)
    selected = dot("cs,sl->cl", picks, jacobian_table).astype(jnp.bfloat16)
    selected = lax.optimization_barrier(selected)
    owned = dot("cl,klx->ckx", selected, background).astype(jnp.bfloat16)
    owned = owned.reshape(channels * mem_dev, columns_dev)
    relay_hot = lax.optimization_barrier(one_hot(relay_cols.reshape(-1), columns_dev))

    def to_partner(array, d):
        return lax.ppermute(array, "tile", [(i, i ^ d) for i in range(n_tile)])

    windows, first = [], 0
    for count in split:
        windows.append((first, first + count * block * mem_dev))
        first = windows[-1][1]
    total = first
    args = me[None], send_slots[0], owned
    early = range(half // 2, half)
    late = [d for d in range(half) if d not in early]
    direct_to = range(half, n_tile) if direct else ()
    near = [None] * half
    sent, seen = pack(*args, [(d, 0, total) for d in early], windows[:-1])
    for d, array in zip(early, sent):
        near[d] = array
    sent, more = pack(
        *args,
        [(d, 0, total) for d in late] + [(d, *windows[-1]) for d in direct_to],
        [],
    )
    for d, array in zip(late, sent):
        near[d] = array
    far = sent[len(late) :]
    seen = seen + more
    for i in range(len(seen)):
        seen[i] = lax.ppermute(seen[i], "tile", mirror)
    near[1:] = [to_partner(near[d], d) for d in range(1, half)]
    far = [to_partner(far[d], half + d) for d in range(len(far))]

    places = footprint.T
    weights = footprint_weight.T
    near_place = places - my_half * half_slots
    far_place = places - (1 - my_half) * half_slots
    mixed_place = jnp.stack([near_place, far_place])
    spread = sum(
        jnp.where(
            mixed_place[:, None, j] == lax.iota(jnp.int32, half_slots)[None, :, None],
            weights[j],
            jnp.zeros((), weights.dtype),
        )
        for j in range(foot)
    ).reshape(2 * half_slots, obs_count)

    shape = (channels, mem_dev, obs_count)
    relayed = relay_pack(relay_hot, seen)
    relayed = lax.all_to_all(
        relayed, "tile", 0, 0, tiled=True, axis_index_groups=halves
    )
    prior = None
    for first, count, others in ((relay, direct, far), (0, relay, [relayed])):
        if count:
            prior = prior_piece(
                shape, block, first, count, near, others,
                spread, channel_bias, place[None], prior,
            )

    weight_cols = lax.dynamic_slice_in_dim(analysis_weights[0], mine * mem_dev, mem_dev, 1)
    mixture = background_mean.astype(jnp.float32)[None]
    for shift in range(n_mem):
        piece = anomalies
        if shift:
            piece = lax.ppermute(anomalies, "mem", [((i + shift) % n_mem, i) for i in range(n_mem)])
        start = lax.rem(mine + shift, n_mem) * mem_dev
        part = lax.dynamic_slice_in_dim(weight_cols, start, mem_dev, 0)
        mixture = mixture + dot("klc,km->mlc", piece, part)
    mixture = mixture.astype(jnp.bfloat16)
    return mixture, prior


def solution(mesh):
    sizes = dict(mesh.shape)
    placed = (
        P("mem", None, "tile"),
        P("tile", None, None),
        P(None, "tile"),
        P("mem", None, "tile"),
        P(),
        P(),
        P("tile", None, None),
        P("tile", None),
        P("tile", None),
        P(),
    )

    def body(*arrays):
        return shards(sizes["tile"], sizes["mem"], *arrays)

    return jax.shard_map(
        body,
        mesh=mesh,
        in_specs=placed,
        out_specs=(P("mem", None, "tile"), P(None, "mem", "tile")),
        check_vma=False,
    )
```
